32 devices in a mesh: lat: 8 (over z, core), lon: 4 (over y, x).
Axes of the slice: x: 2, y: 2, z: 4, core: 2. Of those that a mesh axis runs over, the one named last changes fastest.
Arguments:
- field: bfloat16 [128, 128, 256], P('lat', 'lon'), may hold values from -6 to 6
- weights: bfloat16 [8, 4, 3072, 3072], P('lat', 'lon'), may hold values from -0.09375 to 0.09375
- strip_ids: int32 [8, 8], P('lat'), may hold values from 0 to 31, as said below
- counts: int32 [8], P('lat'), may hold values from 2 to 8, as said below
Outputs:
- remapped: bfloat16 [32768, 256], P(('lat', 'lon'))
The draws below stay inside these ranges and needn't reach their ends.
Inputs may be any that keep to these rules, and one draw needn't show every extreme that they name: `strip_ids`: row b holds consecutive global strip numbers, the last one repeated where the run meets the end of its window, all among the strips of source bands b - 2 to b + 2, band c holding strips 4 * c to 4 * c + 3. Band b uses the first counts[b] slots of its row.
All inputs are finite; a program needn't handle non-finite values.
Results may differ from the reference program's by a relative error of at most 0.0059.
Values may be sent and summed in bfloat16 or wider, within the bound.
A program may use at most 64 MiB of HBM per device.

```python
import jax
import jax.numpy as jnp
from jax import lax

CHANNELS = 256
SRC_ROWS = 16
SRC_LON = 32
STRIP_ROWS = 4
STRIP_CELLS = 128
SLOTS = 8
REACH = 2
TGT_DEV = 1024
TGT_WIN = 3072
NUM_LAT = 128
NUM_LON = 128
NUM_TGT = 32768
N_LAT = 8
N_LON = 4


def strip_plan(key):
    per_device = SRC_ROWS // STRIP_ROWS
    strip_total = N_LAT * per_device
    band_index = jnp.arange(N_LAT, dtype=jnp.int32)
    lower = jnp.maximum(0, (band_index - REACH) * per_device)
    upper = jnp.minimum(strip_total, (band_index + REACH + 1) * per_device)
    drawn = jax.random.randint(jax.random.fold_in(key, 11), (N_LAT,), 2, SLOTS + 1)
    pattern = band_index % 4
    forced = (pattern == 0) | (pattern == 2)
    used = jnp.where(forced, SLOTS, drawn)
    room = upper - lower - used + 1
    offset = jax.random.randint(jax.random.fold_in(key, 12), (N_LAT,), 0, room)
    first_strip = lower + offset
    first_strip = jnp.where(pattern == 0, lower, jnp.where(pattern == 2, upper - SLOTS, first_strip))
    slot_range = jnp.arange(SLOTS, dtype=jnp.int32)
    chosen = jnp.minimum(first_strip[:, None] + slot_range[None, :], upper[:, None] - 1)
    return (chosen.astype(jnp.int32), used.astype(jnp.int32))


def draw_strip_ids(key, part):
    return strip_plan(key)[0]


def draw_counts(key, part):
    return strip_plan(key)[1]


def level_of(own_key, dims, shards, least, top_value):
    level, own = 1.0, jax.random.fold_in(own_key, 6)
    for position, parts in shards:
        draws = jnp.exp(jax.random.uniform(jax.random.fold_in(own, position), (parts,), jnp.float32, least / len(shards), top_value / len(shards)))
        level = level * jnp.repeat(draws, dims[position] // parts).reshape([-1 if axis == position else 1 for axis in range(len(dims))])
    return level


def normal_values(stream_key, shape, deviation, limit, shards=(), kind=jnp.bfloat16):
    values = jax.random.normal(stream_key, shape, jnp.float32) * deviation
    if len(shards) > 0:
        values = level_of(stream_key, shape, shards, -0.22, 0.18) * values
    return jnp.clip(values, min=-limit, max=limit).astype(kind)


def setup_inputs(seed: int = 0) -> dict:
    seeds = jax.random.split(jax.random.key(seed), 5)
    return {
        "field": normal_values(seeds[0], (NUM_LAT, NUM_LON, CHANNELS), 1.0, 6.0, ((0, 8), (1, 4))),
        "weights": normal_values(seeds[1], (N_LAT, N_LON, TGT_WIN, SLOTS * 3 * STRIP_CELLS), (3 * STRIP_CELLS * SLOTS * 3 // 2) ** -0.5, 0.09375, ((0, 8), (1, 4))),
        "strip_ids": draw_strip_ids(jax.random.fold_in(seeds[4], 71), 0),
        "counts": draw_counts(jax.random.fold_in(seeds[4], 71), 0),
    }


def reference(field, weights, strip_ids, counts):
    lon_wrapped = jnp.concatenate([field[:, -1:], field, field[:, :1]], axis=1)
    padded = jnp.concatenate([lon_wrapped[:1], lon_wrapped, lon_wrapped[-1:]], axis=0)
    values = padded.astype(jnp.float32)
    eastward = ((values[1:-1, 2:] - values[1:-1, :-2]) * 0.5).astype(jnp.bfloat16)
    northward = ((values[2:, 1:-1] - values[:-2, 1:-1]) * 0.5).astype(jnp.bfloat16)
    strip_total = NUM_LAT // STRIP_ROWS

    def sectorize(component):
        shaped = component.reshape(strip_total, STRIP_ROWS, N_LON, SRC_LON, CHANNELS)
        return shaped.transpose(0, 2, 1, 3, 4).reshape(strip_total, N_LON, STRIP_CELLS, CHANNELS)

    strips = jnp.stack([sectorize(field), sectorize(eastward), sectorize(northward)], axis=2)
    strips = strips.reshape(strip_total, N_LON, 3 * STRIP_CELLS, CHANNELS)
    slot_range = jnp.arange(SLOTS, dtype=jnp.int32)

    def band_rows(band_index):
        chosen = jnp.take(strips, strip_ids[band_index].astype(jnp.int32), axis=0)
        live_slots = slot_range < counts[band_index]
        chosen = jnp.where(live_slots[:, None, None, None], chosen, jnp.zeros_like(chosen))
        chosen = chosen.transpose(1, 0, 2, 3).reshape(N_LON, SLOTS * 3 * STRIP_CELLS, CHANNELS)
        weights_band = weights[band_index]

        def sector_partial(sector, collected):
            result = jnp.dot(weights_band[sector], chosen[sector], preferred_element_type=jnp.float32)
            return collected.at[sector].set(result)

        collected = lax.fori_loop(0, N_LON, sector_partial, jnp.zeros((N_LON, TGT_WIN, CHANNELS), jnp.float32))
        blocks = collected.reshape(N_LON, 3, TGT_DEV, CHANNELS)
        total = blocks[:, 1] + jnp.roll(blocks[:, 2], 1, axis=0) + jnp.roll(blocks[:, 0], -1, axis=0)
        return total.astype(jnp.bfloat16)

    mapped = lax.map(band_rows, jnp.arange(N_LAT, dtype=jnp.int32))
    return mapped.reshape(NUM_TGT, CHANNELS)
```

```python
import functools

import jax
import jax.numpy as jnp
from jax import lax
from jax.experimental import pallas as pl
from jax.experimental.pallas import tpu as pltpu
from jax.sharding import PartitionSpec as P

STRIP_ROWS = 4
REACH = 2
LANES = 128
CHUNKS = 4
SUB = 2
PIECES = CHUNKS * SUB
MESH = pl.DeviceIdType.MESH
F32 = jnp.float32
BF16 = jnp.bfloat16


def kernel(
    n_lat, n_lon, field, weights, ids_hbm, counts_hbm, out,
    ids, counts, win, edge_f, edge, relayed, ghost, ghost_f, wv, picked, near, own, out_a, out_b, in_a, in_b,
    table_sem, w_sem, own_sem, know, tile_send, tile_recv, fwd_send, row_send, row_recv,
    turn_send, turn_recv, ghost_send, ghost_recv, a_send, a_recv, b_send, b_recv,
):
    b = lax.axis_index("lat")
    s = lax.axis_index("lon")
    rows, lons, chans = field.shape
    halves = chans // LANES
    slots = ids_hbm.shape[1]
    third = weights.shape[2] // 3
    part = third // CHUNKS
    piece = part // SUB
    odd = lax.rem(b, 2)
    partner = b + 1 - 2 * odd
    s_odd = lax.rem(s, 2)
    bands = 2 * REACH + 1

    def lon_at(step):
        return lax.rem(s + step + n_lon, n_lon)

    def valid(band):
        return jnp.logical_and(band >= 0, band < n_lat)

    def place(offset):
        return (offset + REACH) * rows + 1

    def lanes(h):
        return pl.ds(h * LANES, LANES)

    far_row = 2 * third * s_odd
    near_row = 2 * third * (1 - s_odd)
    far_to = lax.rem(s + n_lon - 2 + 4 * s_odd, n_lon)
    near_to = lax.rem(s + n_lon + 1 - 2 * s_odd, n_lon)

    own_loads = [
        pltpu.make_async_copy(field.at[:, :, lanes(h)], win[h].at[pl.ds(place(0), rows)], own_sem.at[h])
        for h in range(halves)
    ]
    for copy in own_loads:
        copy.start()
    tables = [
        pltpu.make_async_copy(ids_hbm, ids, table_sem.at[0]),
        pltpu.make_async_copy(counts_hbm, counts, table_sem.at[1]),
    ]
    for table in tables:
        table.start()

    def each_peer(act):
        for offset in (-2, -1, 1, 2):
            @pl.when(valid(b + offset))
            def _():
                act(b + offset, s)
        third_band = b + 3 - 6 * odd

        @pl.when(valid(third_band))
        def _():
            act(third_band, s)
        act(b, near_to)
        act(b, lon_at(-2))
        act(b, lon_at(2))

    peers = 3 + valid(b + 3 - 6 * odd).astype(jnp.int32)
    for offset in (-2, -1, 1, 2):
        peers = peers + valid(b + offset).astype(jnp.int32)

    barrier = pltpu.get_barrier_semaphore()
    each_peer(lambda band, sector: pl.semaphore_signal(
        barrier, inc=1, device_id=(band, sector), device_id_type=MESH))

    loads = []
    for i, start in enumerate((far_row, near_row, third)):
        span = pl.ds(pl.multiple_of(start, third), third)
        loads.append(pltpu.make_async_copy(weights.at[0, 0, span], wv.at[span], w_sem.at[i]))
        loads[i].start()

    for h in range(halves):
        own_loads[h].wait()
        for r in range(rows):
            cells = win[h][place(0) + r].astype(F32)
            edge_f[0, h, pl.ds(r, 1), :] = cells[lons - 1 :]
            edge_f[1, h, pl.ds(r, 1), :] = cells[:1]
        for side in range(2):
            edge[side, h] = edge_f[side, h].astype(BF16)
    pl.semaphore_wait(barrier, peers)

    each_peer(lambda band, sector: pl.semaphore_signal(
        know, inc=1, device_id=(band, sector), device_id_type=MESH))

    def remote(src, dst, send, recv, band, sector):
        return pltpu.make_async_remote_copy(
            src_ref=src, dst_ref=dst, send_sem=send, recv_sem=recv,
            device_id=(band, sector), device_id_type=MESH,
        )

    def tile_copy(kind, h):
        delta = (partner - b, REACH, -REACH)[kind]
        return remote(
            win[h].at[pl.ds(place(0), rows)], win[h].at[pl.ds(place(-delta), rows)],
            tile_send.at[kind, h], tile_recv.at[kind, h], b + delta, s,
        )

    def forward_copy(h):
        offset = REACH - 2 * REACH * odd
        return remote(
            win[h].at[pl.ds(place(offset), rows)], win[h].at[pl.ds(place(offset + b - partner), rows)],
            fwd_send.at[h], tile_recv.at[3, h], partner, s,
        )

    def row_copy(kind, h):
        if kind == 0:
            src, dst, band = win[h].at[pl.ds(place(0) + rows - 1, 1)], win[h].at[pl.ds(0, 1)], b + REACH + 1
        else:
            src, dst, band = win[h].at[pl.ds(place(0), 1)], win[h].at[pl.ds(bands * rows + 1, 1)], b - REACH - 1
        return remote(src, dst, row_send.at[kind, h], row_recv.at[kind, h], band, s)

    def turn_copy(h):
        return remote(edge.at[1 - s_odd, h], relayed.at[h], turn_send.at[h], turn_recv.at[h], b, far_to)

    def ghost_copy(kind, h, offset):
        src, side = ((edge.at[s_odd, h], s_odd), (relayed.at[h], 1 - s_odd))[kind]
        return remote(
            src, ghost.at[side, h, pl.ds((REACH - offset) * rows, rows)],
            ghost_send.at[kind, h, offset + REACH], ghost_recv.at[kind, h, REACH - offset],
            b + offset, near_to,
        )

    def each_tile(h, act):
        for kind, delta in ((1, REACH), (2, -REACH)):
            @pl.when(valid(b + delta))
            def _():
                act(tile_copy(kind, h))
        act(tile_copy(0, h))

    def each_row(h, act):
        for kind, delta in ((0, REACH + 1), (1, -REACH - 1)):
            @pl.when(valid(b + delta))
            def _():
                act(row_copy(kind, h))

    def each_ghost(kind, h, act):
        for offset in range(-REACH, REACH + 1):
            @pl.when(valid(b + offset))
            def _():
                act(ghost_copy(kind, h, offset))

    each_tile(0, lambda copy: copy.start())
    for h in range(halves):
        turn_copy(h).start()
    pl.semaphore_wait(know, peers)
    each_ghost(0, 0, lambda copy: copy.start())
    each_row(0, lambda copy: copy.start())
    turn_copy(0).wait_recv()
    each_ghost(1, 0, lambda copy: copy.start())
    each_tile(1, lambda copy: copy.start())
    each_row(1, lambda copy: copy.start())
    each_ghost(0, 1, lambda copy: copy.start())
    turn_copy(1).wait_recv()
    each_ghost(1, 1, lambda copy: copy.start())

    forwards = valid(b + REACH - 2 * REACH * odd)
    receives = valid(b - 1 + 2 * odd)

    def pass_on(h):
        @pl.when(valid(b - REACH))
        def _():
            tile_copy(1, h).wait_recv()

        @pl.when(valid(b + REACH))
        def _():
            tile_copy(2, h).wait_recv()

        @pl.when(forwards)
        def _():
            forward_copy(h).start()

    def settle(h):
        tile_copy(0, h).wait_recv()

        @pl.when(valid(b - REACH - 1))
        def _():
            row_copy(0, h).wait_recv()

        @pl.when(valid(b + REACH + 1))
        def _():
            row_copy(1, h).wait_recv()

        for offset in range(-REACH, REACH + 1):
            @pl.when(valid(b + offset))
            def _():
                for kind in range(2):
                    ghost_copy(kind, h, -offset).wait_recv()
        for side in range(2):
            ghost_f[side, h] = ghost[side, h].astype(F32)

        @pl.when(receives)
        def _():
            forward_copy(h).wait_recv()

    first_row = place(0) - b * rows
    last_row = first_row + n_lat * rows - 1
    cell = lax.broadcasted_iota(jnp.int32, (lons, LANES), 0)
    depth = STRIP_ROWS * lons
    for table in tables:
        table.wait()
    live_count = counts[0]

    def pick(h):
        for k in range(slots):
            live = jnp.full((lons, LANES), k < live_count)
            start = ids[0, k] * STRIP_ROWS + first_row
            for j in range(STRIP_ROWS):
                at = jnp.clip(start + j, 1, bands * rows)
                centre = win[h][at].astype(F32)
                above = win[h][jnp.maximum(at - 1, first_row)].astype(F32)
                below = win[h][jnp.minimum(at + 1, last_row)].astype(F32)
                west = jnp.where(cell == 0, ghost_f[0, h, pl.ds(at - 1, 1), :], pltpu.roll(centre, 1, 0))
                east = jnp.where(cell == lons - 1, ghost_f[1, h, pl.ds(at - 1, 1), :], pltpu.roll(centre, lons - 1, 0))
                for c, value in enumerate((centre, (east - west) * 0.5, (below - above) * 0.5)):
                    span = pl.ds((3 * k + c) * depth + j * lons, lons)
                    picked[span, lanes(h)] = jnp.where(live, value, 0.0).astype(BF16)

    def product(start, i, columns):
        span = pl.ds(pl.multiple_of(start + i * part, part), part)
        return jnp.dot(wv[span, :], picked[:, columns], preferred_element_type=F32)

    def a_copy(h, j):
        return remote(out_a.at[h, j], in_a.at[h, j], a_send.at[h, j], a_recv.at[h, j], b, far_to)

    def b_copy(h, j):
        return remote(out_b.at[h, j], in_b.at[h, j], b_send.at[h, j], b_recv.at[h, j], b, near_to)

    def far(h, i):
        value = product(far_row, i, lanes(h)).astype(BF16)
        for u in range(SUB):
            out_a[h, i * SUB + u] = value[u * piece : (u + 1) * piece]
            a_copy(h, i * SUB + u).start()

    def beside(i):
        near[pl.ds(pl.multiple_of(i * part, part), part), :] = product(near_row, i, slice(None))

    def relay(h, j):
        a_copy(h, j).wait_recv()
        span = pl.ds(pl.multiple_of(j * piece, piece), piece)
        out_b[h, j] = (near[span, lanes(h)] + in_a[h, j].astype(F32)).astype(BF16)
        b_copy(h, j).start()

    def inner(i):
        own[pl.ds(pl.multiple_of(i * part, part), part), :] = product(third, i, slice(None))

    def finish(h, j):
        b_copy(h, j).wait_recv()
        span = pl.ds(pl.multiple_of(j * piece, piece), piece)
        out[span, lanes(h)] = (own[span, lanes(h)] + in_b[h, j].astype(F32)).astype(BF16)

    def steps(first, last, act):
        def step(i, carry):
            act(i)
            return carry
        lax.fori_loop(first, last, step, 0)

    def far_and_relay(i):
        far(1, i)
        relay(0, i + 1)

    def inner_and_relay(i):
        inner(i)
        relay(0, i + 1 + CHUNKS)

    def relay_and_finish(j):
        relay(1, j)
        finish(0, j)

    pass_on(0)
    settle(0)
    pick(0)
    loads[0].wait()
    steps(0, CHUNKS, functools.partial(far, 0))
    pass_on(1)
    settle(1)
    pick(1)
    loads[1].wait()
    steps(0, CHUNKS - 1, beside)
    relay(0, 0)
    beside(CHUNKS - 1)
    steps(0, CHUNKS, far_and_relay)
    loads[2].wait()
    steps(0, CHUNKS - 1, inner_and_relay)
    inner(CHUNKS - 1)
    steps(0, PIECES, relay_and_finish)
    steps(0, PIECES, functools.partial(finish, 1))

    for h in range(halves):
        turn_copy(h).wait_send()
        for kind in range(2):
            each_ghost(kind, h, lambda copy: copy.wait_send())
        each_row(h, lambda copy: copy.wait_send())
        each_tile(h, lambda copy: copy.wait_send())

        @pl.when(forwards)
        def _():
            forward_copy(h).wait_send()

        for j in range(PIECES):
            a_copy(h, j).wait_send()
            b_copy(h, j).wait_send()


def solution(mesh):
    n_lat, n_lon = mesh.shape["lat"], mesh.shape["lon"]

    def body(field, weights, strip_ids, counts):
        rows, lons, chans = field.shape
        tall, wide = weights.shape[2:]
        third = tall // 3
        piece = third // PIECES
        halves = chans // LANES
        bands = 2 * REACH + 1
        dma = pltpu.SemaphoreType.DMA
        block = (halves, PIECES, piece, LANES)
        return pl.pallas_call(
            functools.partial(kernel, n_lat, n_lon),
            out_shape=pltpu.VMEM((third, chans), BF16),
            in_specs=[
                pl.BlockSpec(memory_space=pl.ANY),
                pl.BlockSpec(memory_space=pl.ANY),
                pl.BlockSpec(memory_space=pl.ANY),
                pl.BlockSpec(memory_space=pl.ANY),
            ],
            out_specs=pl.BlockSpec(memory_space=pltpu.VMEM),
            scratch_shapes=[
                pltpu.SMEM(strip_ids.shape, jnp.int32),
                pltpu.SMEM(counts.shape, jnp.int32),
                [pltpu.VMEM((bands * rows + 2, lons, LANES), BF16) for _ in range(halves)],
                pltpu.VMEM((2, halves, rows, LANES), F32),
                pltpu.VMEM((2, halves, rows, LANES), BF16),
                pltpu.VMEM((halves, rows, LANES), BF16),
                pltpu.VMEM((2, halves, bands * rows, LANES), BF16),
                pltpu.VMEM((2, halves, bands * rows, LANES), F32),
                pltpu.VMEM((tall, wide), BF16),
                pltpu.VMEM((wide, chans), BF16),
                pltpu.VMEM((third, chans), F32),
                pltpu.VMEM((third, chans), F32),
                pltpu.VMEM(block, BF16),
                pltpu.VMEM(block, BF16),
                pltpu.VMEM(block, BF16),
                pltpu.VMEM(block, BF16),
                dma((2,)),
                dma((3,)),
                dma((halves,)),
                pltpu.SemaphoreType.REGULAR,
                dma((3, halves)),
                dma((4, halves)),
                dma((halves,)),
                dma((2, halves)),
                dma((2, halves)),
                dma((halves,)),
                dma((halves,)),
                dma((2, halves, bands)),
                dma((2, halves, bands)),
                dma((halves, PIECES)),
                dma((halves, PIECES)),
                dma((halves, PIECES)),
                dma((halves, PIECES)),
            ],
            compiler_params=pltpu.CompilerParams(collective_id=0, has_side_effects=True),
        )(field, weights, strip_ids, counts)

    placed = (P("lat", "lon", None), P("lat", "lon", None, None), P("lat", None), P("lat"))
    return jax.shard_map(
        body, mesh=mesh, in_specs=placed, out_specs=P(("lat", "lon"), None), check_vma=False
    )
```

```python
import functools

import jax
import jax.numpy as jnp
from jax import lax
from jax.experimental import pallas as pl
from jax.experimental.pallas import tpu as pltpu
from jax.sharding import PartitionSpec as P

STRIP_ROWS = 4
REACH = 2
LANES = 128
CHUNKS = 4
MESH = pl.DeviceIdType.MESH
F32 = jnp.float32
BF16 = jnp.bfloat16


def kernel(
    n_lat, n_lon, field, weights, ids_hbm, counts_hbm, out,
    ids, counts, win, edge_f, edge, relayed, ghost, ghost_f, wv, picked, near, own, out_a, out_b, in_a, in_b,
    table_sem, w_sem, own_sem, know, tile_send, tile_recv, fwd_send, row_send, row_recv,
    turn_send, turn_recv, ghost_send, ghost_recv, a_send, a_recv, b_send, b_recv,
):
    b = lax.axis_index("lat")
    s = lax.axis_index("lon")
    rows, lons, chans = field.shape
    halves = chans // LANES
    slots = ids_hbm.shape[1]
    third = weights.shape[2] // 3
    part = third // CHUNKS
    odd = lax.rem(b, 2)
    partner = b + 1 - 2 * odd
    s_odd = lax.rem(s, 2)
    bands = 2 * REACH + 1

    def lon_at(step):
        return lax.rem(s + step + n_lon, n_lon)

    def valid(band):
        return jnp.logical_and(band >= 0, band < n_lat)

    def place(offset):
        return (offset + REACH) * rows + 1

    def lanes(h):
        return pl.ds(h * LANES, LANES)

    far_row = 2 * third * s_odd
    near_row = 2 * third * (1 - s_odd)
    far_to = lax.rem(s + n_lon - 2 + 4 * s_odd, n_lon)
    near_to = lax.rem(s + n_lon + 1 - 2 * s_odd, n_lon)

    own_loads = [
        pltpu.make_async_copy(field.at[:, :, lanes(h)], win[h].at[pl.ds(place(0), rows)], own_sem.at[h])
        for h in range(halves)
    ]
    for copy in own_loads:
        copy.start()
    tables = [
        pltpu.make_async_copy(ids_hbm, ids, table_sem.at[0]),
        pltpu.make_async_copy(counts_hbm, counts, table_sem.at[1]),
    ]
    for table in tables:
        table.start()

    def each_peer(act):
        for offset in (-2, -1, 1, 2):
            @pl.when(valid(b + offset))
            def _():
                act(b + offset, s)
        third_band = b + 3 - 6 * odd

        @pl.when(valid(third_band))
        def _():
            act(third_band, s)
        act(b, near_to)
        act(b, lon_at(-2))
        act(b, lon_at(2))

    peers = 3 + valid(b + 3 - 6 * odd).astype(jnp.int32)
    for offset in (-2, -1, 1, 2):
        peers = peers + valid(b + offset).astype(jnp.int32)

    barrier = pltpu.get_barrier_semaphore()
    each_peer(lambda band, sector: pl.semaphore_signal(
        barrier, inc=1, device_id=(band, sector), device_id_type=MESH))

    loads = []
    for i, start in enumerate((far_row, near_row, third)):
        span = pl.ds(pl.multiple_of(start, third), third)
        loads.append(pltpu.make_async_copy(weights.at[0, 0, span], wv.at[span], w_sem.at[i]))
        loads[i].start()

    for h in range(halves):
        own_loads[h].wait()
        for r in range(rows):
            cells = win[h][place(0) + r].astype(F32)
            edge_f[0, h, pl.ds(r, 1), :] = cells[lons - 1 :]
            edge_f[1, h, pl.ds(r, 1), :] = cells[:1]
        for side in range(2):
            edge[side, h] = edge_f[side, h].astype(BF16)
    pl.semaphore_wait(barrier, peers)

    each_peer(lambda band, sector: pl.semaphore_signal(
        know, inc=1, device_id=(band, sector), device_id_type=MESH))

    def remote(src, dst, send, recv, band, sector):
        return pltpu.make_async_remote_copy(
            src_ref=src, dst_ref=dst, send_sem=send, recv_sem=recv,
            device_id=(band, sector), device_id_type=MESH,
        )

    def tile_copy(kind, h):
        delta = (partner - b, REACH, -REACH)[kind]
        return remote(
            win[h].at[pl.ds(place(0), rows)], win[h].at[pl.ds(place(-delta), rows)],
            tile_send.at[kind, h], tile_recv.at[kind, h], b + delta, s,
        )

    def forward_copy(h):
        offset = REACH - 2 * REACH * odd
        return remote(
            win[h].at[pl.ds(place(offset), rows)], win[h].at[pl.ds(place(offset + b - partner), rows)],
            fwd_send.at[h], tile_recv.at[3, h], partner, s,
        )

    def row_copy(kind, h):
        if kind == 0:
            src, dst, band = win[h].at[pl.ds(place(0) + rows - 1, 1)], win[h].at[pl.ds(0, 1)], b + REACH + 1
        else:
            src, dst, band = win[h].at[pl.ds(place(0), 1)], win[h].at[pl.ds(bands * rows + 1, 1)], b - REACH - 1
        return remote(src, dst, row_send.at[kind, h], row_recv.at[kind, h], band, s)

    def turn_copy(h):
        return remote(edge.at[1 - s_odd, h], relayed.at[h], turn_send.at[h], turn_recv.at[h], b, far_to)

    def ghost_copy(kind, h, offset):
        src, side = ((edge.at[s_odd, h], s_odd), (relayed.at[h], 1 - s_odd))[kind]
        return remote(
            src, ghost.at[side, h, pl.ds((REACH - offset) * rows, rows)],
            ghost_send.at[kind, h, offset + REACH], ghost_recv.at[kind, h, REACH - offset],
            b + offset, near_to,
        )

    def each_tile(h, act):
        for kind, delta in ((1, REACH), (2, -REACH)):
            @pl.when(valid(b + delta))
            def _():
                act(tile_copy(kind, h))
        act(tile_copy(0, h))

    def each_row(h, act):
        for kind, delta in ((0, REACH + 1), (1, -REACH - 1)):
            @pl.when(valid(b + delta))
            def _():
                act(row_copy(kind, h))

    def each_ghost(kind, h, act):
        for offset in (-2, 2, -1, 1, 0):
            @pl.when(valid(b + offset))
            def _():
                act(ghost_copy(kind, h, offset))

    each_tile(0, lambda copy: copy.start())
    for h in range(halves):
        turn_copy(h).start()
    pl.semaphore_wait(know, peers)
    each_ghost(0, 0, lambda copy: copy.start())
    each_row(0, lambda copy: copy.start())
    turn_copy(0).wait_recv()
    each_ghost(1, 0, lambda copy: copy.start())
    each_tile(1, lambda copy: copy.start())
    each_row(1, lambda copy: copy.start())
    each_ghost(0, 1, lambda copy: copy.start())
    turn_copy(1).wait_recv()
    each_ghost(1, 1, lambda copy: copy.start())

    forwards = valid(b + REACH - 2 * REACH * odd)
    receives = valid(b - 1 + 2 * odd)

    def pass_on(h):
        @pl.when(forwards)
        def _():
            @pl.when(odd == 0)
            def _():
                tile_copy(2, h).wait_recv()

            @pl.when(odd == 1)
            def _():
                tile_copy(1, h).wait_recv()
            forward_copy(h).start()

    def settle(h):
        tile_copy(0, h).wait_recv()

        @pl.when(jnp.logical_and(odd == 0, valid(b - REACH)))
        def _():
            tile_copy(1, h).wait_recv()

        @pl.when(jnp.logical_and(odd == 1, valid(b + REACH)))
        def _():
            tile_copy(2, h).wait_recv()

        @pl.when(valid(b - REACH - 1))
        def _():
            row_copy(0, h).wait_recv()

        @pl.when(valid(b + REACH + 1))
        def _():
            row_copy(1, h).wait_recv()

        for offset in range(-REACH, REACH + 1):
            @pl.when(valid(b + offset))
            def _():
                for kind in range(2):
                    ghost_copy(kind, h, -offset).wait_recv()
        for side in range(2):
            ghost_f[side, h] = ghost[side, h].astype(F32)

        @pl.when(receives)
        def _():
            forward_copy(h).wait_recv()

    first_row = place(0) - b * rows
    last_row = first_row + n_lat * rows - 1
    cell = lax.broadcasted_iota(jnp.int32, (lons, LANES), 0)
    depth = STRIP_ROWS * lons
    for table in tables:
        table.wait()
    live_count = counts[0]

    def pick(h):
        for k in range(slots):
            live = jnp.full((lons, LANES), k < live_count)
            start = ids[0, k] * STRIP_ROWS + first_row
            for j in range(STRIP_ROWS):
                at = jnp.clip(start + j, 1, bands * rows)
                centre = win[h][at].astype(F32)
                above = win[h][jnp.maximum(at - 1, first_row)].astype(F32)
                below = win[h][jnp.minimum(at + 1, last_row)].astype(F32)
                west = jnp.where(cell == 0, ghost_f[0, h, pl.ds(at - 1, 1), :], pltpu.roll(centre, 1, 0))
                east = jnp.where(cell == lons - 1, ghost_f[1, h, pl.ds(at - 1, 1), :], pltpu.roll(centre, lons - 1, 0))
                for c, value in enumerate((centre, (east - west) * 0.5, (below - above) * 0.5)):
                    span = pl.ds((3 * k + c) * depth + j * lons, lons)
                    picked[span, lanes(h)] = jnp.where(live, value, 0.0).astype(BF16)

    def product(start, i, columns):
        span = pl.ds(pl.multiple_of(start + i * part, part), part)
        return jnp.dot(wv[span, :], picked[:, columns], preferred_element_type=F32)

    last = halves - 1
    small = part // 2

    def piece(i):
        return pl.multiple_of(i * part, part), part, i

    first = [(u * small, small, CHUNKS * u) for u in range(2)]
    split = [((CHUNKS - 1) * part + u * small, small, CHUNKS - 1 + u) for u in range(2)]

    def a_copy(h, piece, to=far_to):
        span = pl.ds(piece[0], piece[1])
        return remote(out_a.at[h, span], in_a.at[h, span], a_send.at[h, piece[2]], a_recv.at[h, piece[2]], b, to)

    def b_copy(h, piece):
        span = pl.ds(piece[0], piece[1])
        return remote(out_b.at[h, span], in_b.at[h, span], b_send.at[h, piece[2]], b_recv.at[h, piece[2]], b, near_to)

    def far(h, i, pieces=None, to=far_to):
        out_a[h, pl.ds(pl.multiple_of(i * part, part), part)] = product(far_row, i, lanes(h)).astype(BF16)
        for item in pieces or [piece(i)]:
            a_copy(h, item, to).start()

    def beside(i):
        near[pl.ds(pl.multiple_of(i * part, part), part), :] = product(near_row, i, slice(None))

    def relay(h, piece):
        a_copy(h, piece).wait_recv()
        span = pl.ds(piece[0], piece[1])
        out_b[h, span] = (near[span, lanes(h)] + in_a[h, span].astype(F32)).astype(BF16)
        b_copy(h, piece).start()

    def inner(i):
        own[pl.ds(pl.multiple_of(i * part, part), part), :] = product(third, i, slice(None))

    def finish(h, piece):
        b_copy(h, piece).wait_recv()
        span = pl.ds(piece[0], piece[1])
        out[span, lanes(h)] = (own[span, lanes(h)] + in_b[h, span].astype(F32)).astype(BF16)

    def steps(first, last, act):
        def step(i, carry):
            act(i)
            return carry
        lax.fori_loop(first, last, step, 0)

    pass_on(0)
    settle(0)
    pick(0)
    loads[0].wait()
    far(0, 0, first)
    steps(1, CHUNKS, functools.partial(far, 0))
    pass_on(1)
    settle(1)
    pick(1)
    loads[1].wait()
    steps(0, CHUNKS - 1, beside)
    relay(0, first[0])
    beside(CHUNKS - 1)
    relay(0, first[1])
    steps(0, CHUNKS - 2, functools.partial(far, last))
    relay(0, piece(1))
    far(last, CHUNKS - 2)
    far(last, CHUNKS - 1, split)
    loads[2].wait()
    relay(0, piece(2))
    steps(0, CHUNKS - 1, inner)
    relay(0, piece(3))
    inner(CHUNKS - 1)
    for i in range(CHUNKS - 1):
        relay(last, piece(i))
        if i == 0:
            for u in range(2):
                finish(0, first[u])
        else:
            finish(0, piece(i))
    for u in range(2):
        relay(last, split[u])
    finish(0, piece(CHUNKS - 1))
    for i in range(CHUNKS - 1):
        finish(last, piece(i))
    for u in range(2):
        finish(last, split[u])

    for h in range(halves):
        turn_copy(h).wait_send()
        for kind in range(2):
            each_ghost(kind, h, lambda copy: copy.wait_send())
        each_row(h, lambda copy: copy.wait_send())
        each_tile(h, lambda copy: copy.wait_send())

        @pl.when(forwards)
        def _():
            forward_copy(h).wait_send()

        for item in (first if h == 0 else split) + [piece(i + (h == 0)) for i in range(CHUNKS - 1)]:
            a_copy(h, item).wait_send()
            b_copy(h, item).wait_send()


def solution(mesh):
    n_lat, n_lon = mesh.shape["lat"], mesh.shape["lon"]

    def body(field, weights, strip_ids, counts):
        rows, lons, chans = field.shape
        tall, wide = weights.shape[2:]
        third = tall // 3
        halves = chans // LANES
        bands = 2 * REACH + 1
        dma = pltpu.SemaphoreType.DMA
        block = (halves, third, LANES)
        return pl.pallas_call(
            functools.partial(kernel, n_lat, n_lon),
            out_shape=pltpu.VMEM((third, chans), BF16),
            in_specs=[
                pl.BlockSpec(memory_space=pl.ANY),
                pl.BlockSpec(memory_space=pl.ANY),
                pl.BlockSpec(memory_space=pl.ANY),
                pl.BlockSpec(memory_space=pl.ANY),
            ],
            out_specs=pl.BlockSpec(memory_space=pltpu.VMEM),
            scratch_shapes=[
                pltpu.SMEM(strip_ids.shape, jnp.int32),
                pltpu.SMEM(counts.shape, jnp.int32),
                [pltpu.VMEM((bands * rows + 2, lons, LANES), BF16) for _ in range(halves)],
                pltpu.VMEM((2, halves, rows, LANES), F32),
                pltpu.VMEM((2, halves, rows, LANES), BF16),
                pltpu.VMEM((halves, rows, LANES), BF16),
                pltpu.VMEM((2, halves, bands * rows, LANES), BF16),
                pltpu.VMEM((2, halves, bands * rows, LANES), F32),
                pltpu.VMEM((tall, wide), BF16),
                pltpu.VMEM((wide, chans), BF16),
                pltpu.VMEM((third, chans), F32),
                pltpu.VMEM((third, chans), F32),
                pltpu.VMEM(block, BF16),
                pltpu.VMEM(block, BF16),
                pltpu.VMEM(block, BF16),
                pltpu.VMEM(block, BF16),
                dma((2,)),
                dma((3,)),
                dma((halves,)),
                pltpu.SemaphoreType.REGULAR,
                dma((3, halves)),
                dma((4, halves)),
                dma((halves,)),
                dma((2, halves)),
                dma((2, halves)),
                dma((halves,)),
                dma((halves,)),
                dma((2, halves, bands)),
                dma((2, halves, bands)),
                dma((halves, CHUNKS + 1)),
                dma((halves, CHUNKS + 1)),
                dma((halves, CHUNKS + 1)),
                dma((halves, CHUNKS + 1)),
            ],
            compiler_params=pltpu.CompilerParams(collective_id=0, has_side_effects=True),
        )(field, weights, strip_ids, counts)

    placed = (P("lat", "lon", None), P("lat", "lon", None, None), P("lat", None), P("lat"))
    return jax.shard_map(
        body, mesh=mesh, in_specs=placed, out_specs=P(("lat", "lon"), None), check_vma=False
    )
```
